256 devices in a mesh: dp: 128 (over z_hi, x, y, core), tensor: 2 (over z_lo).
Axes of the slice: x: 4, y: 4, z: 8 (z_hi: 4, z_lo: 2; z = z_hi * 2 + z_lo), core: 2. Of those that a mesh axis runs over, the one named last changes fastest.
Arguments:
- tokens: bfloat16 [16384, 1792], P('dp'), may hold values from -6 to 6
- targets: bfloat16 [16384, 1792], P('dp'), may hold values from -6 to 6
- live_mask: int32 [16384], P('dp'), may hold values from 0 to 1, as said below
- up_weight: bfloat16 [1792, 7168], P('dp', 'tensor'), may hold values from -0.125 to 0.125
- down_weight: bfloat16 [1792, 7168], P('dp', 'tensor'), may hold values from -0.0625 to 0.0625
- probe_rows: int32 [1792], replicated, may hold values from 0 to 16777215
- probe_cols: int32 [7168], P('tensor'), may hold values from 0 to 16777215
- moment: float32 [1792, 512], P('dp', 'tensor'), may hold values from 0.01 to 1
Outputs:
- hess_diag: float32 [1792, 512], P('dp', 'tensor')
- second_moment: float32 [1792, 512], P('dp', 'tensor')
- mean_loss: float32 [], replicated
The draws below stay inside these ranges and needn't reach their ends.
Inputs may be any that keep to these rules, and one draw needn't show every extreme that they name: In every aligned block of 128 tokens the first token has live_mask 1.
All inputs are finite; a program needn't handle non-finite values.
Results may differ from the reference program's by a relative error of at most 0.0023.
Values may be sent and summed in bfloat16 or wider, within the bound.
No kernel may reach another device: no remote copies, remote signals or barrier semaphores. Data moves between devices by JAX's collectives and lax.ppermute only.
A program may use at most 128 MiB of HBM per device.

```python
import math
import jax
import jax.numpy as jnp
from jax import lax

D = 1792
FF = 7168
BLOCK = 14
TOK_DEV = 128
TOKENS = 16384


def draw_live_mask(key, part):
    group_id = jnp.arange(TOKENS) // TOK_DEV
    group_count = TOKENS // TOK_DEV
    threshold = 300 + 600 * group_id // max(group_count - 1, 1)
    dice_rolls = jax.random.randint(key, (TOKENS,), 0, 1000)
    live_rows = (dice_rolls < threshold).astype(jnp.int32)
    lead_rows = (jnp.arange(TOKENS) % TOK_DEV == 0).astype(jnp.int32)
    return jnp.maximum(live_rows, lead_rows)


def place_ends(array, rng, low, top_value):
    longest = array.shape.index(max(array.shape))
    spots = []
    for shift in (0, 1):
        where = [jax.random.randint(jax.random.fold_in(rng, axis), (), 0, length) for axis, length in enumerate(array.shape)]
        where[longest] = (where[longest] + shift) % array.shape[longest]
        spots.append(tuple(where))
    return array.at[spots[0]].set(low).at[spots[1]].set(top_value)


def block_levels(stream_key, dims, shards, low, high):
    loudness = 1.0
    for axis_at, blocks in shards:
        steps = jax.random.uniform(jax.random.fold_in(jax.random.fold_in(stream_key, 6), axis_at), (blocks,), jnp.float32, low / len(shards), high / len(shards))
        loudness = loudness * jnp.repeat(jnp.exp(steps), dims[axis_at] // blocks).reshape((-1,) + (1,) * (len(dims) - 1 - axis_at))
    return loudness


def bell_draw(rng, extent, spread, bound, split=(), held_as=jnp.bfloat16):
    level = block_levels(rng, extent, split, -0.22, 0.18) if split else 1.0
    values = jax.random.normal(rng, extent, jnp.float32) * spread * level
    return jnp.minimum(jnp.maximum(values, -bound), bound).astype(held_as)


def setup_inputs(seed: int = 0) -> dict:
    streams_of = jax.random.split(jax.random.key(seed), 9)
    return {
        "tokens": bell_draw(streams_of[0], (TOKENS, D), 1.0, 6.0, ((0, 128),)),
        "targets": bell_draw(streams_of[1], (TOKENS, D), 1.0, 6.0, ((0, 128),)),
        "live_mask": draw_live_mask(jax.random.fold_in(streams_of[8], 71), 0),
        "up_weight": bell_draw(streams_of[3], (D, FF), D ** -0.5, 0.125, ((0, 128), (1, 2))),
        "down_weight": bell_draw(streams_of[4], (D, FF), FF ** -0.5, 0.0625, ((0, 128), (1, 2))),
        "probe_rows": place_ends(jax.random.randint(streams_of[5], (D,), 0, 16777216), jax.random.fold_in(streams_of[5], 1), 0, 16777215).astype(jnp.int32),
        "probe_cols": place_ends(jax.random.randint(streams_of[6], (FF,), 0, 16777216), jax.random.fold_in(streams_of[6], 1), 0, 16777215).astype(jnp.int32),
        "moment": jnp.clip(jnp.exp(math.log(1.0) - 4.6051702 * jax.random.uniform(streams_of[7], (D, FF // BLOCK), jnp.float32) ** block_levels(streams_of[7], (D, FF // BLOCK), ((0, 128), (1, 2)), -0.2, 0.2)), 0.01, 1.0),
    }


gelu_coef = 0.7978845608028654
cubic_coef = 0.044715
beta_two = 0.999


def probe_signs(row_keys, col_keys):
    hashed = jnp.bitwise_xor(row_keys[:, None] * 747796405, col_keys[None, :])
    hashed = jnp.bitwise_xor(hashed, jnp.right_shift(hashed, 15) & 131071)
    hashed = hashed * 695872825
    hashed = jnp.bitwise_xor(hashed, jnp.right_shift(hashed, 13) & 524287)
    hashed = hashed * 739982445
    hashed = jnp.bitwise_xor(hashed, jnp.right_shift(hashed, 16) & 65535)
    parity = jnp.right_shift(hashed, 11) & 1
    return (2 * parity - 1).astype(jnp.bfloat16)


def gelu_parts(preact):
    tanh_arg = gelu_coef * (preact + cubic_coef * preact * preact * preact)
    tanh_val = jnp.tanh(tanh_arg)
    sech_sq = 1.0 - tanh_val * tanh_val
    arg_slope = gelu_coef * (1.0 + 3.0 * cubic_coef * preact * preact)
    arg_curve = gelu_coef * 6.0 * cubic_coef * preact
    gelu_value = 0.5 * preact * (1.0 + tanh_val)
    gelu_slope = 0.5 * (1.0 + tanh_val) + 0.5 * preact * sech_sq * arg_slope
    gelu_curve = sech_sq * (arg_slope - preact * tanh_val * arg_slope * arg_slope + 0.5 * preact * arg_curve)
    return gelu_value, gelu_slope, gelu_curve


def reference(tokens, targets, live_mask, up_weight, down_weight, probe_rows, probe_cols, moment):
    probe = probe_signs(probe_rows, probe_cols)
    count = jnp.sum(live_mask.astype(jnp.float32))
    group_total = TOKENS // TOK_DEV
    tok_blocks = tokens.reshape(group_total, TOK_DEV, D)
    tgt_blocks = targets.reshape(group_total, TOK_DEV, D)
    mask_blocks = live_mask.reshape(group_total, TOK_DEV)

    def token_block(running, blocks):
        acc_curv, acc_loss = running
        inputs, wanted, mask_rows = blocks
        preact = jnp.dot(inputs, up_weight, preferred_element_type=jnp.float32)
        tangent = jnp.dot(inputs, probe, preferred_element_type=jnp.float32)
        gelu_value, gelu_slope, gelu_curve = gelu_parts(preact)
        hidden = gelu_value.astype(jnp.bfloat16)
        hidden_dir = (gelu_slope * tangent).astype(jnp.bfloat16)
        outputs = jnp.dot(hidden, down_weight.T, preferred_element_type=jnp.float32)
        out_dir = jnp.dot(hidden_dir, down_weight.T, preferred_element_type=jnp.float32)
        live_rows = mask_rows.astype(jnp.float32)[:, None]
        diff = outputs - wanted.astype(jnp.float32)
        weighted = live_rows * diff
        loss_part = jnp.sum(weighted * diff)
        residual = weighted.astype(jnp.bfloat16)
        residual_dir = (live_rows * out_dir).astype(jnp.bfloat16)
        grad_h = jnp.dot(residual, down_weight, preferred_element_type=jnp.float32)
        grad_dir = jnp.dot(residual_dir, down_weight, preferred_element_type=jnp.float32)
        chain_grad = (grad_dir * gelu_slope + grad_h * gelu_curve * tangent).astype(jnp.bfloat16)
        curv_part = jnp.dot(inputs.T, chain_grad, preferred_element_type=jnp.float32)
        return (acc_curv + curv_part, acc_loss + loss_part), None

    start_state = (jnp.zeros((D, FF), jnp.float32), jnp.zeros((), jnp.float32))
    final_state, _ = lax.scan(token_block, start_state, (tok_blocks, tgt_blocks, mask_blocks))
    curv_sum, loss_sum = final_state
    hutch_terms = probe.astype(jnp.float32) * curv_sum
    hess_diag = hutch_terms.reshape(D, FF // BLOCK, BLOCK).mean(axis=-1) / count
    second_moment = beta_two * moment + (1.0 - beta_two) * hess_diag * hess_diag
    mean_loss = loss_sum / (2.0 * count)
    return hess_diag, second_moment, mean_loss
```

```python
import jax
import jax.numpy as jnp
from jax import lax
from jax.experimental import pallas as pl
from jax.experimental.pallas import tpu as pltpu
from jax.sharding import Mesh
from jax.sharding import PartitionSpec as P

BLOCK = 14
DP = ("zh", "x", "y", "c")
GROUP = ("x", "y", "zh")
SWAP = [(0, 1), (1, 0)]
UP = [(i, (i + 1) % 4) for i in range(4)]
DOWN = [(i, (i - 1) % 4) for i in range(4)]
CHUNKS = 2

gelu_coef = 0.7978845608028654
cubic_coef = 0.044715
beta_two = 0.999


def probe_signs(row_keys, col_keys):
    hashed = jnp.bitwise_xor(row_keys[:, None] * 747796405, col_keys[None, :])
    hashed = jnp.bitwise_xor(hashed, jnp.right_shift(hashed, 15) & 131071)
    hashed = hashed * 695872825
    hashed = jnp.bitwise_xor(hashed, jnp.right_shift(hashed, 13) & 524287)
    hashed = hashed * 739982445
    hashed = jnp.bitwise_xor(hashed, jnp.right_shift(hashed, 16) & 65535)
    parity = jnp.right_shift(hashed, 11) & 1
    return (2 * parity - 1).astype(jnp.bfloat16)


def gelu_parts(preact):
    tanh_arg = gelu_coef * (preact + cubic_coef * preact * preact * preact)
    tanh_val = jnp.tanh(tanh_arg)
    sech_sq = 1.0 - tanh_val * tanh_val
    arg_slope = gelu_coef * (1.0 + 3.0 * cubic_coef * preact * preact)
    arg_curve = gelu_coef * 6.0 * cubic_coef * preact
    gelu_value = 0.5 * preact * (1.0 + tanh_val)
    gelu_slope = 0.5 * (1.0 + tanh_val) + 0.5 * preact * sech_sq * arg_slope
    gelu_curve = sech_sq * (
        arg_slope - preact * tanh_val * arg_slope * arg_slope + 0.5 * preact * arg_curve
    )
    return gelu_value, gelu_slope, gelu_curve


def pieces_of_ring(chunk, axis, cut):
    prev = lax.ppermute(chunk, axis, UP)
    nxt = lax.ppermute(chunk, axis, DOWN)
    far_low = lax.ppermute(prev[:cut], axis, UP)
    far_high = lax.ppermute(nxt[cut:], axis, DOWN)
    return chunk, nxt, (far_low, far_high), prev


def in_order(pieces, axis):
    own, nxt, far, prev = pieces
    me = lax.axis_index(axis)
    far = jnp.concatenate(far, axis=0)
    return jnp.stack(
        [
            jnp.where(
                me == k,
                own,
                jnp.where(me == (k - 1) % 4, nxt, jnp.where(me == (k - 2) % 4, far, prev)),
            )
            for k in range(4)
        ]
    )


def over_plane(chunk):
    rows, width = chunk.shape
    half = rows // 2
    x, y = lax.axis_index("x"), lax.axis_index("y")
    along_x = in_order(pieces_of_ring(chunk[:half], "x", 24), "x")
    along_y = in_order(pieces_of_ring(chunk[half:], "y", 24), "y")
    own_a, nxt_a, (low_a, high_a), prev_a = pieces_of_ring(along_x, "y", 2)
    own_b, nxt_b, (low_b, high_b), prev_b = pieces_of_ring(along_y, "x", 2)
    whole = jnp.zeros((4, 4, 2, half, width), chunk.dtype)

    def put_a(whole, piece, first, step):
        return lax.dynamic_update_slice(whole, piece[:, None, None], (first, (y + step) % 4, 0, 0, 0))

    def put_b(whole, piece, first, step):
        return lax.dynamic_update_slice(whole, piece[None, :, None], ((x + step) % 4, first, 1, 0, 0))

    for put, own, nxt, low, high, prev in (
        (put_a, own_a, nxt_a, low_a, high_a, prev_a),
        (put_b, own_b, nxt_b, low_b, high_b, prev_b),
    ):
        whole = put(whole, own, 0, 0)
        whole = put(whole, nxt, 0, 1)
        whole = put(whole, prev, 0, 3)
        whole = put(whole, low, 0, 2)
        whole = put(whole, high, 2, 2)
    return whole.reshape(16 * rows, width)


def by_plane(array):
    lead = array.shape[:-1]
    parts = array.reshape(*lead, 4, 16, -1)
    return jnp.swapaxes(parts, -3, -2).reshape(array.shape)


def curvature_kernel(tok_ref, chain_ref, sign_ref, pick_ref, out_ref):
    product = jnp.dot(tok_ref[...], chain_ref[...], preferred_element_type=jnp.float32)
    signed = product * sign_ref[...].astype(jnp.float32)
    high = signed.astype(jnp.bfloat16)
    low = (signed - high.astype(jnp.float32)).astype(jnp.bfloat16)
    pick = pick_ref[...]
    out_ref[...] = jnp.dot(high, pick, preferred_element_type=jnp.float32) + jnp.dot(
        low, pick, preferred_element_type=jnp.float32
    )


def block_sums(tok_cols, chain, signs, picker):
    rows, toks = tok_cols.shape
    width = chain.shape[1]
    blocks = picker.shape[1]
    tile = 256
    return pl.pallas_call(
        curvature_kernel,
        grid=(rows // tile,),
        in_specs=[
            pl.BlockSpec((tile, toks), lambda i: (i, 0)),
            pl.BlockSpec((toks, width), lambda i: (0, 0)),
            pl.BlockSpec((tile, width), lambda i: (i, 0)),
            pl.BlockSpec((width, blocks), lambda i: (0, 0)),
        ],
        out_specs=pl.BlockSpec((tile, blocks), lambda i: (i, 0)),
        out_shape=jax.ShapeDtypeStruct((rows, blocks), jnp.float32),
        compiler_params=pltpu.CompilerParams(
            dimension_semantics=("arbitrary",), vmem_limit_bytes=40 * 1024 * 1024
        ),
    )(tok_cols, chain, signs, picker)


def body(tokens, targets, live_mask, up_weight, down_weight, probe_rows, probe_cols, moment):
    tok_count = tokens.shape[0]
    own_rows = up_weight.shape[0]
    width = up_weight.shape[1] // 2
    blocks = width // BLOCK
    c = lax.axis_index("c")
    live_rows = live_mask.astype(jnp.float32)

    def my_half(a, other):
        return jnp.where((c == 0) != other, a[..., :width], a[..., width:])

    def cores_in_order(own, got, axis):
        return jnp.where(
            c == 0, jnp.concatenate([own, got], axis), jnp.concatenate([got, own], axis)
        )

    pairs = []
    for weight in (up_weight, down_weight):
        got = lax.ppermute(my_half(weight, True), "c", SWAP)
        pairs.append(cores_in_order(my_half(weight, False), got, 0))
    up_chunk, down_chunk = (
        in_order(pieces_of_ring(pair, "zh", 16), "zh").reshape(8 * own_rows, width) for pair in pairs
    )
    down = lax.all_gather(down_chunk, ("x", "y"), axis=0, tiled=True)
    up = over_plane(up_chunk)

    own_toks = by_plane(tokens)
    toks = jnp.concatenate([own_toks, lax.ppermute(own_toks, "c", SWAP)], axis=0)
    tok_cols = toks.T
    wanted = by_plane(targets).astype(jnp.float32)
    signs = probe_signs(
        by_plane(probe_rows), lax.dynamic_slice_in_dim(probe_cols, c * width, width)
    )
    unit = lax.broadcasted_iota(jnp.int32, (width, blocks), 0)
    first = BLOCK * lax.broadcasted_iota(jnp.int32, (width, blocks), 1)
    picker = ((unit >= first) & (unit < first + BLOCK)).astype(jnp.bfloat16)

    tangent = jnp.dot(toks, signs, preferred_element_type=jnp.float32)
    preact = jnp.dot(toks, up, preferred_element_type=jnp.float32)
    gelu_value, gelu_slope, gelu_curve = gelu_parts(preact)
    hidden = gelu_value.astype(jnp.bfloat16)
    hidden_dir = (gelu_slope * tangent).astype(jnp.bfloat16)
    bend = gelu_curve * tangent

    size = tok_count // CHUNKS
    loss = jnp.zeros((), jnp.float32)
    chain_own, chain_got = [], []
    for j in range(CHUNKS):
        own = slice(j * size, (j + 1) * size)
        got = slice(tok_count + j * size, tok_count + (j + 1) * size)
        stacked = jnp.concatenate([hidden[own], hidden_dir[own], hidden[got], hidden_dir[got]], axis=0)
        projected = lax.dot_general(
            stacked, down, (((1,), (1,)), ((), ())), preferred_element_type=jnp.float32
        )
        partial = projected[: 2 * size] + lax.ppermute(projected[2 * size :], "c", SWAP)
        rounded = partial.astype(jnp.bfloat16)
        kept = lax.reduce_precision(partial, 8, 7)
        total = kept + lax.ppermute(rounded, "t", SWAP).astype(jnp.float32)
        live = live_rows[own][:, None]
        diff = total[:size] - wanted[own]
        weighted = live * diff
        loss = loss + jnp.sum(weighted * diff)
        residual = jnp.concatenate([weighted, live * total[size:]], axis=0).astype(jnp.bfloat16)
        residuals = jnp.concatenate([residual, lax.ppermute(residual, "c", SWAP)], axis=0)
        back = jnp.dot(residuals, down, preferred_element_type=jnp.float32)
        for at, rows, keep in ((0, own, chain_own), (2 * size, got, chain_got)):
            grad_h = back[at : at + size]
            grad_dir = back[at + size : at + 2 * size]
            keep.append((grad_dir * gelu_slope[rows] + grad_h * bend[rows]).astype(jnp.bfloat16))
    chain_grad = jnp.concatenate(chain_own + chain_got, axis=0)

    sums = block_sums(tok_cols, chain_grad, signs, picker)
    lane = lax.broadcasted_iota(jnp.int32, (64, 4, blocks), 2)
    extra = jnp.where(lane == 0, loss, jnp.where(lane == 1, jnp.sum(live_rows), 0.0))
    tiles = jnp.concatenate([sums.reshape(64, 2 * own_rows, blocks), extra], axis=1)
    shared = jnp.sum(lax.all_to_all(tiles, GROUP, 0, 0, tiled=True), axis=0)
    tail = shared[2 * own_rows :]
    mine = jnp.where(c == 0, shared[:own_rows], shared[own_rows : 2 * own_rows])
    other = jnp.where(c == 0, shared[own_rows : 2 * own_rows], shared[:own_rows])
    got = lax.ppermute(jnp.concatenate([other, tail[:2]], axis=0), "c", SWAP)
    own_share = cores_in_order(mine, got[:own_rows], 1) * (1.0 / BLOCK)
    loss_sum = tail[0, 0] + got[own_rows, 0]
    total_count = tail[0, 1] + got[own_rows, 1]
    hess_diag = own_share / total_count
    second_moment = beta_two * moment + (1.0 - beta_two) * hess_diag * hess_diag
    mean_loss = loss_sum / (2.0 * total_count)
    return hess_diag, second_moment, mean_loss


def solution(mesh):
    torus = Mesh(mesh.devices.reshape(4, 4, 4, 2, 2), (*DP, "t"))
    placed = (
        P(DP, None),
        P(DP, None),
        P(DP),
        P(DP, "t"),
        P(DP, "t"),
        P(),
        P("t"),
        P(DP, "t"),
    )
    return jax.shard_map(
        body,
        mesh=torus,
        in_specs=placed,
        out_specs=(P(DP, "t"), P(DP, "t"), P()),
        check_vma=False,
    )
```

```python
import jax
import jax.numpy as jnp
from jax import lax
from jax.experimental import pallas as pl
from jax.experimental.pallas import tpu as pltpu
from jax.sharding import Mesh
from jax.sharding import PartitionSpec as P

BLOCK = 14
DP = ("zh", "x", "y", "c")
SWAP = [(0, 1), (1, 0)]
UP = [(i, (i + 1) % 4) for i in range(4)]
CHUNKS = 4
DOWN = [(i, (i - 1) % 4) for i in range(4)]

gelu_coef = 0.7978845608028654
cubic_coef = 0.044715
beta_two = 0.999


def probe_signs(row_keys, col_keys):
    hashed = jnp.bitwise_xor(row_keys[:, None] * 747796405, col_keys[None, :])
    hashed = jnp.bitwise_xor(hashed, jnp.right_shift(hashed, 15) & 131071)
    hashed = hashed * 695872825
    hashed = jnp.bitwise_xor(hashed, jnp.right_shift(hashed, 13) & 524287)
    hashed = hashed * 739982445
    hashed = jnp.bitwise_xor(hashed, jnp.right_shift(hashed, 16) & 65535)
    parity = jnp.right_shift(hashed, 11) & 1
    return (2 * parity - 1).astype(jnp.bfloat16)


def gelu_parts(preact):
    tanh_arg = gelu_coef * (preact + cubic_coef * preact * preact * preact)
    tanh_val = jnp.tanh(tanh_arg)
    sech_sq = 1.0 - tanh_val * tanh_val
    arg_slope = gelu_coef * (1.0 + 3.0 * cubic_coef * preact * preact)
    arg_curve = gelu_coef * 6.0 * cubic_coef * preact
    gelu_value = 0.5 * preact * (1.0 + tanh_val)
    gelu_slope = 0.5 * (1.0 + tanh_val) + 0.5 * preact * sech_sq * arg_slope
    gelu_curve = sech_sq * (
        arg_slope - preact * tanh_val * arg_slope * arg_slope + 0.5 * preact * arg_curve
    )
    return gelu_value, gelu_slope, gelu_curve


def pieces_of_ring(chunk, axis, cut):
    prev = lax.ppermute(chunk, axis, UP)
    nxt = lax.ppermute(chunk, axis, DOWN)
    far_low = lax.ppermute(prev[:cut], axis, UP)
    far_high = lax.ppermute(nxt[cut:], axis, DOWN)
    return chunk, nxt, (far_low, far_high), prev


def in_order(pieces, axis):
    own, nxt, far, prev = pieces
    me = lax.axis_index(axis)
    far = jnp.concatenate(far, axis=0)
    return jnp.stack(
        [
            jnp.where(
                me == k,
                own,
                jnp.where(me == (k - 1) % 4, nxt, jnp.where(me == (k - 2) % 4, far, prev)),
            )
            for k in range(4)
        ]
    )


def first_phase(chunk):
    half = chunk.shape[0] // 2
    along_x = pieces_of_ring(chunk[:half], "x", 24)
    along_y = pieces_of_ring(chunk[half:], "y", 24)
    return along_x, along_y


def second_phase(along_x, along_y):
    first = pieces_of_ring(in_order(along_x, "x"), "y", 2)
    second = pieces_of_ring(in_order(along_y, "y"), "x", 2)
    own_a, nxt_a, far_a, prev_a = first
    own_b, nxt_b, far_b, prev_b = second
    width = own_a.shape[-1]
    return [
        jnp.concatenate(group, axis=0).reshape(-1, width)
        for group in ((own_a, own_b), (nxt_a, nxt_b, prev_a, prev_b), (*far_a, *far_b))
    ]


def plane_groups(columns):
    width = columns.shape[-1]
    parts = columns.reshape(4, 4, 2, -1, width)
    x, y = lax.axis_index("x"), lax.axis_index("y")

    def first(step):
        return lax.dynamic_index_in_dim(parts[:, :, 0], (y + step) & 3, 1, False)

    def second(step):
        return lax.dynamic_index_in_dim(parts[:, :, 1], (x + step) & 3, 0, False)

    return [
        jnp.concatenate(group, axis=0).reshape(-1, width)
        for group in (
            (first(0), second(0)),
            (first(1), second(1), first(3), second(3)),
            (first(2), second(2)),
        )
    ]


def after(arrays, *others):
    return lax.optimization_barrier((arrays, others))[0]


def by_plane(columns):
    parts = columns.reshape(4, 16, -1, columns.shape[-1])
    return jnp.swapaxes(parts, 0, 1).reshape(columns.shape)


def curvature_kernel(tok_ref, chain_ref, sign_ref, pick_ref, out_ref):
    product = jnp.dot(tok_ref[...], chain_ref[...], preferred_element_type=jnp.float32)
    signed = product * sign_ref[...].astype(jnp.float32)
    high = signed.astype(jnp.bfloat16)
    low = (signed - high.astype(jnp.float32)).astype(jnp.bfloat16)
    pick = pick_ref[...]
    out_ref[...] = jnp.dot(high, pick, preferred_element_type=jnp.float32) + jnp.dot(
        low, pick, preferred_element_type=jnp.float32
    )


def block_sums(tok_cols, chain, signs, picker):
    rows, toks = tok_cols.shape
    width = chain.shape[1]
    blocks = picker.shape[1]
    tile = 256
    return pl.pallas_call(
        curvature_kernel,
        grid=(rows // tile,),
        in_specs=[
            pl.BlockSpec((tile, toks), lambda i: (i, 0)),
            pl.BlockSpec((toks, width), lambda i: (0, 0)),
            pl.BlockSpec((tile, width), lambda i: (i, 0)),
            pl.BlockSpec((width, blocks), lambda i: (0, 0)),
        ],
        out_specs=pl.BlockSpec((tile, blocks), lambda i: (i, 0)),
        out_shape=jax.ShapeDtypeStruct((rows, blocks), jnp.float32),
        compiler_params=pltpu.CompilerParams(
            dimension_semantics=("arbitrary",), vmem_limit_bytes=40 * 1024 * 1024
        ),
    )(tok_cols, chain, signs, picker)


def body(tokens, targets, live_mask, up_weight, down_weight, probe_rows, probe_cols, moment):
    tok_count = tokens.shape[0]
    own_rows = up_weight.shape[0]
    width = up_weight.shape[1] // 2
    blocks = width // BLOCK
    c = lax.axis_index("c")
    live_rows = live_mask.astype(jnp.float32)

    def my_half(a, other):
        return jnp.where((c == 0) != other, a[..., :width], a[..., width:])

    def cores_in_order(own, got, axis):
        return jnp.where(
            c == 0, jnp.concatenate([own, got], axis), jnp.concatenate([got, own], axis)
        )

    both = jnp.stack([up_weight, down_weight])
    got = lax.ppermute(my_half(both, True), "c", SWAP)
    ring = pieces_of_ring(cores_in_order(my_half(both, False), got, 1), "zh", 1)
    chunks = in_order(ring, "zh")
    up_chunk = chunks[:, 0].reshape(8 * own_rows, width)
    down_chunk = chunks[:, 1].reshape(8 * own_rows, width)
    whole_down = lax.all_gather(down_chunk, ("x", "y"), axis=0, tiled=True)
    up_x, up_y = first_phase(up_chunk)
    tokens, targets, probe_rows = after((tokens, targets, probe_rows), up_x[2], up_y[2])
    ups = second_phase(up_x, up_y)

    own_cols = tokens.T
    tok_cols = jnp.concatenate([own_cols, lax.ppermute(own_cols, "c", SWAP)], axis=1)
    wanted = by_plane(targets.T)
    signs = probe_signs(probe_rows, lax.dynamic_slice_in_dim(probe_cols, c * width, width))
    unit = lax.broadcasted_iota(jnp.int32, (width, blocks), 0)
    first = BLOCK * lax.broadcasted_iota(jnp.int32, (width, blocks), 1)
    picker = ((unit >= first) & (unit < first + BLOCK)).astype(jnp.bfloat16)

    def by_features(a, b):
        return lax.dot_general(a, b, (((0,), (0,)), ((), ())), preferred_element_type=jnp.float32)

    tangent = by_features(tok_cols, signs)
    preact = sum(by_features(t, w) for t, w in zip(plane_groups(by_plane(tok_cols)), ups))
    gelu_value, gelu_slope, gelu_curve = gelu_parts(preact)
    hidden = gelu_value.astype(jnp.bfloat16)
    hidden_dir = (gelu_slope * tangent).astype(jnp.bfloat16)
    bend = gelu_curve * tangent
    n = tok_count
    stacked = jnp.concatenate([hidden[:n], hidden_dir[:n], hidden[n:], hidden_dir[n:]], axis=0)

    loss = jnp.zeros((), jnp.float32)
    live = live_rows[None, :]
    back = jnp.zeros((4 * n, width), jnp.float32)
    size = whole_down.shape[0] // CHUNKS
    for k in range(CHUNKS):
        down = whole_down[k * size : (k + 1) * size]
        want = wanted[k * size : (k + 1) * size]
        projected = lax.dot_general(
            down, stacked, (((1,), (1,)), ((), ())), preferred_element_type=jnp.float32
        )
        partial = projected[:, : 2 * n] + lax.ppermute(projected[:, 2 * n :], "c", SWAP)
        kept = lax.reduce_precision(partial, 8, 7)
        total = kept + lax.ppermute(partial.astype(jnp.bfloat16), "t", SWAP).astype(jnp.float32)
        diff = total[:, :n] - want.astype(jnp.float32)
        weighted = live * diff
        loss = loss + jnp.sum(weighted * diff)
        residual = jnp.concatenate([weighted, live * total[:, n:]], axis=1).astype(jnp.bfloat16)
        residuals = jnp.concatenate([residual, lax.ppermute(residual, "c", SWAP)], axis=1)
        back = back + by_features(residuals, down)
    chain_grad = jnp.concatenate(
        [
            back[at + n : at + 2 * n] * gelu_slope[rows] + back[at : at + n] * bend[rows]
            for at, rows in ((0, slice(0, n)), (2 * n, slice(n, 2 * n)))
        ],
        axis=0,
    ).astype(jnp.bfloat16)

    sums = block_sums(tok_cols, chain_grad, signs, picker)
    tiles = jnp.swapaxes(sums.reshape(4, 16, 2, own_rows, blocks), 0, 1)
    lane = lax.broadcasted_iota(jnp.int32, (16, 4, 2, 16 - own_rows, blocks), 4)
    loss_high = lax.reduce_precision(loss, 8, 7)
    extra = jnp.where(
        lane == 0,
        loss_high,
        jnp.where(lane == 1, jnp.sum(live_rows), jnp.where(lane == 2, loss - loss_high, 0.0)),
    )
    tiles = jnp.concatenate([tiles, extra], axis=3).astype(jnp.bfloat16)
    shared = lax.all_to_all(tiles, ("x", "y"), 0, 0, tiled=True)
    shared = jnp.sum(shared.astype(jnp.float32), axis=0).reshape(8, 16, blocks)
    shared = lax.all_to_all(shared, ("zh", "c"), 0, 0, tiled=True)
    shared = jnp.sum(shared.reshape(4, 2, 16, blocks), axis=0)
    own_share = jnp.concatenate([shared[0, :own_rows], shared[1, :own_rows]], axis=1) * (1.0 / BLOCK)
    ends = shared[0, own_rows] + shared[1, own_rows]
    loss_sum = ends[0] + ends[2]
    total_count = ends[1]
    hess_diag = own_share / total_count
    second_moment = beta_two * moment + (1.0 - beta_two) * hess_diag * hess_diag
    mean_loss = loss_sum / (2.0 * total_count)
    return hess_diag, second_moment, mean_loss


def solution(mesh):
    torus = Mesh(mesh.devices.reshape(4, 4, 4, 2, 2), (*DP, "t"))
    placed = (
        P(DP, None),
        P(DP, None),
        P(DP),
        P(DP, "t"),
        P(DP, "t"),
        P(),
        P("t"),
        P(DP, "t"),
    )
    return jax.shard_map(
        body,
        mesh=torus,
        in_specs=placed,
        out_specs=(P(DP, "t"), P(DP, "t"), P()),
        check_vma=False,
    )
```

```python
import jax
import jax.numpy as jnp
from jax import lax
from jax.experimental import pallas as pl
from jax.experimental.pallas import tpu as pltpu
from jax.sharding import Mesh
from jax.sharding import PartitionSpec as P


BLOCK = 14
DP = ("zh", "x", "y", "c")
SWAP = [(0, 1), (1, 0)]
UP = [(i, (i + 1) % 4) for i in range(4)]
CHUNKS = 4
DOWN = [(i, (i - 1) % 4) for i in range(4)]

gelu_coef = 0.7978845608028654
cubic_coef = 0.044715
beta_two = 0.999


def probe_signs(row_keys, col_keys):
    hashed = jnp.bitwise_xor(row_keys[:, None] * 747796405, col_keys[None, :])
    hashed = jnp.bitwise_xor(hashed, jnp.right_shift(hashed, 15) & 131071)
    hashed = hashed * 695872825
    hashed = jnp.bitwise_xor(hashed, jnp.right_shift(hashed, 13) & 524287)
    hashed = hashed * 739982445
    hashed = jnp.bitwise_xor(hashed, jnp.right_shift(hashed, 16) & 65535)
    parity = jnp.right_shift(hashed, 11) & 1
    return (2 * parity - 1).astype(jnp.bfloat16)


def gelu_parts(preact):
    tanh_arg = gelu_coef * (preact + cubic_coef * preact * preact * preact)
    tanh_val = jnp.tanh(tanh_arg)
    sech_sq = 1.0 - tanh_val * tanh_val
    arg_slope = gelu_coef * (1.0 + 3.0 * cubic_coef * preact * preact)
    arg_curve = gelu_coef * 6.0 * cubic_coef * preact
    gelu_value = 0.5 * preact * (1.0 + tanh_val)
    gelu_slope = 0.5 * (1.0 + tanh_val) + 0.5 * preact * sech_sq * arg_slope
    gelu_curve = sech_sq * (
        arg_slope - preact * tanh_val * arg_slope * arg_slope + 0.5 * preact * arg_curve
    )
    return gelu_value, gelu_slope, gelu_curve


def pieces_of_ring(chunk, axis, cut):
    prev = lax.ppermute(chunk, axis, UP)
    nxt = lax.ppermute(chunk, axis, DOWN)
    far_low = lax.ppermute(prev[:cut], axis, UP)
    far_high = lax.ppermute(nxt[cut:], axis, DOWN)
    return chunk, nxt, (far_low, far_high), prev


def in_order(pieces, axis):
    own, nxt, far, prev = pieces
    me = lax.axis_index(axis)
    far = jnp.concatenate(far, axis=0)
    return jnp.stack(
        [
            jnp.where(
                me == k,
                own,
                jnp.where(me == (k - 1) % 4, nxt, jnp.where(me == (k - 2) % 4, far, prev)),
            )
            for k in range(4)
        ]
    )


def first_phase(chunk):
    half = chunk.shape[0] // 2
    along_x = pieces_of_ring(chunk[:half], "x", 24)
    along_y = pieces_of_ring(chunk[half:], "y", 24)
    return along_x, along_y


def second_phase(along_x, along_y):
    first = pieces_of_ring(in_order(along_x, "x"), "y", 2)
    second = pieces_of_ring(in_order(along_y, "y"), "x", 2)
    own_a, nxt_a, far_a, prev_a = first
    own_b, nxt_b, far_b, prev_b = second
    width = own_a.shape[-1]
    groups = [
        jnp.concatenate(group, axis=0).reshape(-1, width)
        for group in ((own_a, own_b), (nxt_a, nxt_b, prev_a, prev_b), (*far_a, *far_b))
    ]
    return groups, (nxt_a, nxt_b, prev_a, prev_b)


def plane_groups(columns):
    width = columns.shape[-1]
    parts = columns.reshape(4, 4, 2, -1, width)
    x, y = lax.axis_index("x"), lax.axis_index("y")

    def first(step):
        return lax.dynamic_index_in_dim(parts[:, :, 0], (y + step) & 3, 1, False)

    def second(step):
        return lax.dynamic_index_in_dim(parts[:, :, 1], (x + step) & 3, 0, False)

    return [
        jnp.concatenate(group, axis=0).reshape(-1, width)
        for group in (
            (first(0), second(0)),
            (first(1), second(1), first(3), second(3)),
            (first(2), second(2)),
        )
    ]


def after(arrays, *others):
    return lax.optimization_barrier((arrays, others))[0]


def by_plane(columns):
    parts = columns.reshape(4, 16, -1, columns.shape[-1])
    return jnp.swapaxes(parts, 0, 1).reshape(columns.shape)


def activation_kernel(pre_ref, tangent_ref, stacked_ref, slope_ref, bend_ref):
    n = pre_ref.shape[0] // 2
    tangent = tangent_ref[...]
    gelu_value, gelu_slope, gelu_curve = gelu_parts(pre_ref[...])
    hidden = gelu_value.astype(jnp.bfloat16)
    hidden_dir = (gelu_slope * tangent).astype(jnp.bfloat16)
    for at, part in enumerate((hidden[:n], hidden_dir[:n], hidden[n:], hidden_dir[n:])):
        stacked_ref[at * n : (at + 1) * n] = part
    slope_ref[...] = gelu_slope
    bend_ref[...] = gelu_curve * tangent


def activations(preact, tangent):
    toks, width = preact.shape
    tile = 256

    def block(rows):
        return pl.BlockSpec((rows, tile), lambda i: (0, i))

    return pl.pallas_call(
        activation_kernel,
        grid=(width // tile,),
        in_specs=[block(toks), block(toks)],
        out_specs=[block(2 * toks), block(toks), block(toks)],
        out_shape=[
            jax.ShapeDtypeStruct((2 * toks, width), jnp.bfloat16),
            jax.ShapeDtypeStruct((toks, width), jnp.float32),
            jax.ShapeDtypeStruct((toks, width), jnp.float32),
        ],
        compiler_params=pltpu.CompilerParams(dimension_semantics=("arbitrary",)),
    )(preact, tangent)


def curvature_kernel(back_ref, slope_ref, bend_ref, tok_ref, sign_ref, pick_ref, out_ref, chain_ref):
    n = slope_ref.shape[0] // 2

    @pl.when(pl.program_id(0) == 0)
    def _():
        for half in range(2):
            rows = pl.ds(half * n, n)
            grad_h = back_ref[pl.ds(2 * half * n, n)]
            grad_dir = back_ref[pl.ds((2 * half + 1) * n, n)]
            chain = grad_dir * slope_ref[rows] + grad_h * bend_ref[rows]
            chain_ref[rows] = chain.astype(jnp.bfloat16)

    product = jnp.dot(tok_ref[...], chain_ref[...], preferred_element_type=jnp.float32)
    signed = product * sign_ref[...].astype(jnp.float32)
    high = signed.astype(jnp.bfloat16)
    low = (signed - high.astype(jnp.float32)).astype(jnp.bfloat16)
    pick = pick_ref[...]
    out_ref[...] = jnp.dot(high, pick, preferred_element_type=jnp.float32) + jnp.dot(
        low, pick, preferred_element_type=jnp.float32
    )


def block_sums(back, slope, bend, tok_cols, signs, picker):
    rows, toks = tok_cols.shape
    width, blocks = picker.shape
    tile = 256

    def whole(a):
        return pl.BlockSpec(a.shape, lambda i: (0, 0))

    return pl.pallas_call(
        curvature_kernel,
        grid=(rows // tile,),
        in_specs=[
            whole(back),
            whole(slope),
            whole(bend),
            pl.BlockSpec((tile, toks), lambda i: (i, 0)),
            pl.BlockSpec((tile, width), lambda i: (i, 0)),
            whole(picker),
        ],
        out_specs=pl.BlockSpec((tile, blocks), lambda i: (i, 0)),
        out_shape=jax.ShapeDtypeStruct((rows, blocks), jnp.float32),
        scratch_shapes=[pltpu.VMEM((toks, width), jnp.bfloat16)],
        compiler_params=pltpu.CompilerParams(
            dimension_semantics=("arbitrary",), vmem_limit_bytes=40 * 1024 * 1024
        ),
    )(back, slope, bend, tok_cols, signs, picker)


def body(tokens, targets, live_mask, up_weight, down_weight, probe_rows, probe_cols, moment):
    tok_count = tokens.shape[0]
    own_rows = up_weight.shape[0]
    width = up_weight.shape[1] // 2
    blocks = width // BLOCK
    c = lax.axis_index("c")
    live_rows = live_mask.astype(jnp.float32)

    def my_half(a, other):
        return jnp.where((c == 0) != other, a[..., :width], a[..., width:])

    def cores_in_order(own, got, axis):
        return jnp.where(
            c == 0, jnp.concatenate([own, got], axis), jnp.concatenate([got, own], axis)
        )

    both = jnp.stack([up_weight, down_weight])
    got = lax.ppermute(my_half(both, True), "c", SWAP)
    ring = pieces_of_ring(cores_in_order(my_half(both, False), got, 1), "zh", 1)
    chunks = in_order(ring, "zh")
    up_chunk = chunks[:, 0].reshape(8 * own_rows, width)
    down_chunk = chunks[:, 1].reshape(8 * own_rows, width)
    whole_down = lax.all_gather(down_chunk, ("x", "y"), axis=0, tiled=True)
    up_x, up_y = first_phase(up_chunk)
    probe_rows = after(probe_rows, up_x[2], up_y[2])
    ups, nearest = second_phase(up_x, up_y)
    tokens, targets = after((tokens, targets), nearest)

    own_cols = tokens.T
    tok_cols = jnp.concatenate([own_cols, lax.ppermute(own_cols, "c", SWAP)], axis=1)
    wanted = by_plane(targets.T)
    signs = probe_signs(probe_rows, lax.dynamic_slice_in_dim(probe_cols, c * width, width))
    signs = lax.optimization_barrier(signs)
    unit = lax.broadcasted_iota(jnp.int32, (width, blocks), 0)
    first = BLOCK * lax.broadcasted_iota(jnp.int32, (width, blocks), 1)
    picker = ((unit >= first) & (unit < first + BLOCK)).astype(jnp.bfloat16)

    def by_features(a, b):
        return lax.dot_general(a, b, (((0,), (0,)), ((), ())), preferred_element_type=jnp.float32)

    tangent = by_features(tok_cols, signs)
    preact = sum(by_features(t, w) for t, w in zip(plane_groups(by_plane(tok_cols)), ups))
    stacked, slope, bend = activations(preact, tangent)
    n = tok_count

    loss = jnp.zeros((), jnp.float32)
    live = live_rows[None, :]
    back = jnp.zeros((4 * n, width), jnp.float32)
    size = whole_down.shape[0] // CHUNKS
    arrived, kept = [], []
    for k in range(CHUNKS):
        projected = lax.dot_general(
            whole_down[k * size : (k + 1) * size],
            stacked,
            (((1,), (1,)), ((), ())),
            preferred_element_type=jnp.float32,
        )
        partial = projected[:, : 2 * n] + lax.ppermute(projected[:, 2 * n :], "c", SWAP)
        kept.append(lax.reduce_precision(partial, 8, 7))
        arrived.append(lax.ppermute(partial.astype(jnp.bfloat16), "t", SWAP))
    for k in range(CHUNKS):
        down = whole_down[k * size : (k + 1) * size]
        want = wanted[k * size : (k + 1) * size]
        got = arrived[k] if k == 0 else after(arrived[k], residual)
        total = kept[k] + got.astype(jnp.float32)
        diff = total[:, :n] - want.astype(jnp.float32)
        weighted = live * diff
        loss = loss + jnp.sum(weighted * diff)
        residual = jnp.concatenate([weighted, live * total[:, n:]], axis=1).astype(jnp.bfloat16)
        residuals = jnp.concatenate([residual, lax.ppermute(residual, "c", SWAP)], axis=1)
        back = back + by_features(residuals, down)
    sums = block_sums(back, slope, bend, tok_cols, signs, picker)
    tiles = jnp.swapaxes(sums.reshape(4, 16, 2, own_rows, blocks), 0, 1)
    lane = lax.broadcasted_iota(jnp.int32, (16, 4, 2, 16 - own_rows, blocks), 4)
    loss_high = lax.reduce_precision(loss, 8, 7)
    extra = jnp.where(
        lane == 0,
        loss_high,
        jnp.where(lane == 1, jnp.sum(live_rows), jnp.where(lane == 2, loss - loss_high, 0.0)),
    )
    tiles = jnp.concatenate([tiles, extra], axis=3).astype(jnp.bfloat16)
    shared = lax.all_to_all(tiles, ("x", "y"), 0, 0, tiled=True)
    shared = jnp.sum(shared.astype(jnp.float32), axis=0).reshape(8, 16, blocks)
    shared = lax.all_to_all(shared, ("zh", "c"), 0, 0, tiled=True)
    shared = jnp.sum(shared.reshape(4, 2, 16, blocks), axis=0)
    own_share = jnp.concatenate([shared[0, :own_rows], shared[1, :own_rows]], axis=1) * (1.0 / BLOCK)
    ends = shared[0, own_rows] + shared[1, own_rows]
    loss_sum = ends[0] + ends[2]
    total_count = ends[1]
    hess_diag = own_share / total_count
    second_moment = beta_two * moment + (1.0 - beta_two) * hess_diag * hess_diag
    mean_loss = loss_sum / (2.0 * total_count)
    return hess_diag, second_moment, mean_loss


def solution(mesh):
    torus = Mesh(mesh.devices.reshape(4, 4, 4, 2, 2), (*DP, "t"))
    placed = (
        P(DP, None),
        P(DP, None),
        P(DP),
        P(DP, "t"),
        P(DP, "t"),
        P(),
        P("t"),
        P(DP, "t"),
    )
    return jax.shard_map(
        body,
        mesh=torus,
        in_specs=placed,
        out_specs=(P(DP, "t"), P(DP, "t"), P()),
        check_vma=False,
    )
```

```python
import jax
import jax.numpy as jnp
from jax import lax
from jax.experimental import pallas as pl
from jax.experimental.pallas import tpu as pltpu
from jax.sharding import Mesh
from jax.sharding import PartitionSpec as P


BLOCK = 14
DP = ("zh", "x", "y", "c")
SWAP = [(0, 1), (1, 0)]
UP = [(i, (i + 1) % 4) for i in range(4)]
CHUNKS = 4
DOWN = [(i, (i - 1) % 4) for i in range(4)]
ACROSS = [(i, (i + 2) % 4) for i in range(4)]

gelu_coef = 0.7978845608028654
cubic_coef = 0.044715
beta_two = 0.999


def probe_signs(row_keys, col_keys):
    hashed = jnp.bitwise_xor(row_keys[:, None] * 747796405, col_keys[None, :])
    hashed = jnp.bitwise_xor(hashed, jnp.right_shift(hashed, 15) & 131071)
    hashed = hashed * 695872825
    hashed = jnp.bitwise_xor(hashed, jnp.right_shift(hashed, 13) & 524287)
    hashed = hashed * 739982445
    hashed = jnp.bitwise_xor(hashed, jnp.right_shift(hashed, 16) & 65535)
    parity = jnp.right_shift(hashed, 11) & 1
    return (2 * parity - 1).astype(jnp.bfloat16)


def gelu_parts(preact):
    tanh_arg = gelu_coef * (preact + cubic_coef * preact * preact * preact)
    tanh_val = jnp.tanh(tanh_arg)
    sech_sq = 1.0 - tanh_val * tanh_val
    arg_slope = gelu_coef * (1.0 + 3.0 * cubic_coef * preact * preact)
    arg_curve = gelu_coef * 6.0 * cubic_coef * preact
    gelu_value = 0.5 * preact * (1.0 + tanh_val)
    gelu_slope = 0.5 * (1.0 + tanh_val) + 0.5 * preact * sech_sq * arg_slope
    gelu_curve = sech_sq * (
        arg_slope - preact * tanh_val * arg_slope * arg_slope + 0.5 * preact * arg_curve
    )
    return gelu_value, gelu_slope, gelu_curve


def pieces_of_ring(chunk, axis, cut):
    prev = lax.ppermute(chunk, axis, UP)
    nxt = lax.ppermute(chunk, axis, DOWN)
    far_low = lax.ppermute(prev[:cut], axis, UP)
    far_high = lax.ppermute(nxt[cut:], axis, DOWN)
    return chunk, nxt, (far_low, far_high), prev


def in_order(pieces, axis):
    own, nxt, far, prev = pieces
    me = lax.axis_index(axis)
    far = jnp.concatenate(far, axis=0)
    return jnp.stack(
        [
            jnp.where(
                me == k,
                own,
                jnp.where(me == (k - 1) % 4, nxt, jnp.where(me == (k - 2) % 4, far, prev)),
            )
            for k in range(4)
        ]
    )


def first_phase(chunk):
    half = chunk.shape[0] // 2
    along_x = pieces_of_ring(chunk[:half], "x", 24)
    along_y = pieces_of_ring(chunk[half:], "y", 24)
    return along_x, along_y


def second_phase(along_x, along_y):
    first = pieces_of_ring(in_order(along_x, "x"), "y", 2)
    second = pieces_of_ring(in_order(along_y, "y"), "x", 2)
    own_a, nxt_a, far_a, prev_a = first
    own_b, nxt_b, far_b, prev_b = second
    width = own_a.shape[-1]
    groups = [
        jnp.concatenate(group, axis=0).reshape(-1, width)
        for group in ((own_a, own_b), (nxt_a, nxt_b, prev_a, prev_b), (*far_a, *far_b))
    ]
    return groups


def plane_groups(columns):
    width = columns.shape[-1]
    parts = columns.reshape(4, 4, 2, -1, width)
    x, y = lax.axis_index("x"), lax.axis_index("y")

    def first(step):
        return lax.dynamic_index_in_dim(parts[:, :, 0], (y + step) & 3, 1, False)

    def second(step):
        return lax.dynamic_index_in_dim(parts[:, :, 1], (x + step) & 3, 0, False)

    return [
        jnp.concatenate(group, axis=0).reshape(-1, width)
        for group in (
            (first(0), second(0)),
            (first(1), second(1), first(3), second(3)),
            (first(2), second(2)),
        )
    ]


def after(arrays, *others):
    return lax.optimization_barrier((arrays, others))[0]


def by_plane(columns):
    parts = columns.reshape(4, 16, -1, columns.shape[-1])
    return jnp.swapaxes(parts, 0, 1).reshape(columns.shape)


def activation_kernel(pre_ref, tangent_ref, stacked_ref, slope_ref, bend_ref):
    n = pre_ref.shape[0] // 2
    tangent = tangent_ref[...]
    gelu_value, gelu_slope, gelu_curve = gelu_parts(pre_ref[...])
    hidden = gelu_value.astype(jnp.bfloat16)
    hidden_dir = (gelu_slope * tangent).astype(jnp.bfloat16)
    for at, part in enumerate((hidden[:n], hidden_dir[:n], hidden[n:], hidden_dir[n:])):
        stacked_ref[at * n : (at + 1) * n] = part
    slope_ref[...] = gelu_slope
    bend_ref[...] = gelu_curve * tangent


def activations(preact, tangent):
    toks, width = preact.shape
    tile = 256

    def block(rows):
        return pl.BlockSpec((rows, tile), lambda i: (0, i))

    return pl.pallas_call(
        activation_kernel,
        grid=(width // tile,),
        in_specs=[block(toks), block(toks)],
        out_specs=[block(2 * toks), block(toks), block(toks)],
        out_shape=[
            jax.ShapeDtypeStruct((2 * toks, width), jnp.bfloat16),
            jax.ShapeDtypeStruct((toks, width), jnp.float32),
            jax.ShapeDtypeStruct((toks, width), jnp.float32),
        ],
        compiler_params=pltpu.CompilerParams(dimension_semantics=("arbitrary",)),
    )(preact, tangent)


def curvature_kernel(back_ref, slope_ref, bend_ref, tok_ref, sign_ref, pick_ref, out_ref, chain_ref):
    n = slope_ref.shape[0] // 2

    @pl.when(pl.program_id(0) == 0)
    def _():
        for half in range(2):
            rows = pl.ds(half * n, n)
            grad_h = back_ref[pl.ds(2 * half * n, n)]
            grad_dir = back_ref[pl.ds((2 * half + 1) * n, n)]
            chain = grad_dir * slope_ref[rows] + grad_h * bend_ref[rows]
            chain_ref[rows] = chain.astype(jnp.bfloat16)

    product = jnp.dot(tok_ref[...], chain_ref[...], preferred_element_type=jnp.float32)
    signed = product * sign_ref[...].astype(jnp.float32)
    high = signed.astype(jnp.bfloat16)
    low = (signed - high.astype(jnp.float32)).astype(jnp.bfloat16)
    pick = pick_ref[...]
    out_ref[...] = jnp.dot(high, pick, preferred_element_type=jnp.float32) + jnp.dot(
        low, pick, preferred_element_type=jnp.float32
    )


def block_sums(back, slope, bend, tok_cols, signs, picker):
    rows, toks = tok_cols.shape
    width, blocks = picker.shape
    tile = 256

    def whole(a):
        return pl.BlockSpec(a.shape, lambda i: (0, 0))

    return pl.pallas_call(
        curvature_kernel,
        grid=(rows // tile,),
        in_specs=[
            whole(back),
            whole(slope),
            whole(bend),
            pl.BlockSpec((tile, toks), lambda i: (i, 0)),
            pl.BlockSpec((tile, width), lambda i: (i, 0)),
            whole(picker),
        ],
        out_specs=pl.BlockSpec((tile, blocks), lambda i: (i, 0)),
        out_shape=jax.ShapeDtypeStruct((rows, blocks), jnp.float32),
        scratch_shapes=[pltpu.VMEM((toks, width), jnp.bfloat16)],
        compiler_params=pltpu.CompilerParams(
            dimension_semantics=("arbitrary",), vmem_limit_bytes=40 * 1024 * 1024
        ),
    )(back, slope, bend, tok_cols, signs, picker)


def body(tokens, targets, live_mask, up_weight, down_weight, probe_rows, probe_cols, moment):
    tok_count = tokens.shape[0]
    own_rows = up_weight.shape[0]
    width = up_weight.shape[1] // 2
    blocks = width // BLOCK
    c = lax.axis_index("c")
    live_rows = live_mask.astype(jnp.float32)

    def my_half(a, other):
        return jnp.where((c == 0) != other, a[..., :width], a[..., width:])

    def cores_in_order(own, got, axis):
        return jnp.where(
            c == 0, jnp.concatenate([own, got], axis), jnp.concatenate([got, own], axis)
        )

    both = jnp.stack([up_weight, down_weight])
    got = lax.ppermute(my_half(both, True), "c", SWAP)
    ring = pieces_of_ring(cores_in_order(my_half(both, False), got, 1), "zh", 1)
    chunks = in_order(ring, "zh")
    up_chunk = chunks[:, 0].reshape(8 * own_rows, width)
    down_chunk = chunks[:, 1].reshape(8 * own_rows, width)
    whole_down = lax.all_gather(down_chunk, ("x", "y"), axis=0, tiled=True)
    up_x, up_y = first_phase(up_chunk)
    tokens, targets, probe_rows = after((tokens, targets, probe_rows), up_x[2], up_y[2])
    ups = second_phase(up_x, up_y)

    toks = jnp.concatenate([tokens, lax.ppermute(tokens, "c", SWAP)], axis=0)
    tok_cols = toks.T
    wanted = by_plane(targets.T)
    signs = probe_signs(probe_rows, lax.dynamic_slice_in_dim(probe_cols, c * width, width))
    signs = lax.optimization_barrier(signs)
    unit = lax.broadcasted_iota(jnp.int32, (width, blocks), 0)
    first = BLOCK * lax.broadcasted_iota(jnp.int32, (width, blocks), 1)
    picker = ((unit >= first) & (unit < first + BLOCK)).astype(jnp.bfloat16)

    def by_features(a, b):
        return lax.dot_general(a, b, (((0,), (0,)), ((), ())), preferred_element_type=jnp.float32)

    tangent = jnp.dot(toks, signs, preferred_element_type=jnp.float32)
    preact = sum(by_features(t, w) for t, w in zip(plane_groups(by_plane(tok_cols)), ups))
    preact, wanted = lax.optimization_barrier((preact, wanted.astype(jnp.float32)))
    stacked, slope, bend = activations(preact, tangent)
    n = tok_count

    loss = jnp.zeros((), jnp.float32)
    live = live_rows[None, :]
    back = jnp.zeros((4 * n, width), jnp.float32)
    size = whole_down.shape[0] // CHUNKS
    arrived, kept = [], []
    for k in range(CHUNKS):
        projected = lax.dot_general(
            whole_down[k * size : (k + 1) * size],
            stacked,
            (((1,), (1,)), ((), ())),
            preferred_element_type=jnp.float32,
        )
        partial = projected[:, : 2 * n] + lax.ppermute(projected[:, 2 * n :], "c", SWAP)
        kept.append(lax.reduce_precision(partial, 8, 7))
        arrived.append(lax.ppermute(partial.astype(jnp.bfloat16), "t", SWAP))
    for k in range(CHUNKS):
        down = whole_down[k * size : (k + 1) * size]
        want = wanted[k * size : (k + 1) * size]
        got = arrived[k] if k == 0 else after(arrived[k], residual)
        total = kept[k] + got.astype(jnp.float32)
        diff = total[:, :n] - want.astype(jnp.float32)
        weighted = live * diff
        loss = loss + jnp.sum(weighted * diff)
        residual = jnp.concatenate([weighted, live * total[:, n:]], axis=1).astype(jnp.bfloat16)
        residuals = jnp.concatenate([residual, lax.ppermute(residual, "c", SWAP)], axis=1)
        back = back + by_features(residuals, down)
    sums = block_sums(back, slope, bend, tok_cols, signs, picker)
    tiles = sums.reshape(4, 16, 2, own_rows, blocks).transpose(1, 2, 0, 3, 4)
    lane = lax.broadcasted_iota(jnp.int32, (16, 2, 4, 16 - own_rows, blocks), 4)
    loss_high = lax.reduce_precision(loss, 8, 7)
    extra = jnp.where(
        lane == 0,
        loss_high,
        jnp.where(lane == 1, jnp.sum(live_rows), jnp.where(lane == 2, loss - loss_high, 0.0)),
    )
    tiles = jnp.concatenate([tiles, extra], axis=3).astype(jnp.bfloat16)
    shared = lax.all_to_all(tiles.reshape(32, 4, 16, blocks), ("x", "y", "c"), 0, 0, tiled=True)
    shared = jnp.sum(shared.reshape(16, 2, 4, 16, blocks).astype(jnp.float32), axis=0)
    zh = lax.axis_index("zh")

    def part_of(step):
        return lax.dynamic_index_in_dim(shared, (zh + step) & 3, 1, False)

    pieces = (
        part_of(0),
        lax.ppermute(part_of(3), "zh", DOWN),
        (lax.ppermute(part_of(2), "zh", ACROSS),),
        lax.ppermute(part_of(1), "zh", UP),
    )
    shared = jnp.sum(in_order(pieces, "zh"), axis=0)
    own_share = jnp.concatenate([shared[0, :own_rows], shared[1, :own_rows]], axis=1) * (1.0 / BLOCK)
    ends = shared[0, own_rows] + shared[1, own_rows]
    loss_sum = ends[0] + ends[2]
    total_count = ends[1]
    hess_diag = own_share / total_count
    second_moment = beta_two * moment + (1.0 - beta_two) * hess_diag * hess_diag
    mean_loss = loss_sum / (2.0 * total_count)
    return hess_diag, second_moment, mean_loss


def solution(mesh):
    torus = Mesh(mesh.devices.reshape(4, 4, 4, 2, 2), (*DP, "t"))
    placed = (
        P(DP, None),
        P(DP, None),
        P(DP),
        P(DP, "t"),
        P(DP, "t"),
        P(),
        P("t"),
        P(DP, "t"),
    )
    return jax.shard_map(
        body,
        mesh=torus,
        in_specs=placed,
        out_specs=(P(DP, "t"), P(DP, "t"), P()),
        check_vma=False,
    )
```
